256 devices in a mesh: slab: 4 (over y), strip: 64 (over z, x, core).
Axes of the slice: x: 4, y: 4, z: 8, core: 2. Of those that a mesh axis runs over, the one named last changes fastest.
Arguments:
- object_field: float32 [2, 8, 1024, 2048], P(None, 'slab', 'strip'), may hold values from -0.5 to 1.5
- first_moment: float32 [2, 8, 1024, 2048], P(None, 'slab', 'strip'), may hold values from -1.8 to 1.8
- second_moment: float32 [2, 8, 1024, 2048], P(None, 'slab', 'strip'), may hold values from 0.001 to 0.1
- probe_wave: float32 [2, 128, 128], replicated, may hold values from -6 to 6
- measured: float32 [256, 128, 128], P('strip'), may hold values from 0 to 4
- positions: int32 [256, 2], replicated, may hold values from 0 to 2047, as said below
- fresnel: float32 [1], replicated, may hold values from 0.002 to 0.02
Outputs:
- object_new: float32 [2, 8, 1024, 2048], P(None, 'slab', 'strip')
- first_new: float32 [2, 8, 1024, 2048], P(None, 'slab', 'strip')
- second_new: float32 [2, 8, 1024, 2048], P(None, 'slab', 'strip')
The draws below stay inside these ranges and needn't reach their ends.
Inputs may be any that keep to these rules, and one draw needn't show every extreme that they name: `positions`: rows 4 d to 4 d + 3 hold (row, column) offsets whose row lies in object rows 16 d to 16 d + 15, for every d; columns lie in 0 to 2047.
All inputs are finite; a program needn't handle non-finite values.
Results may differ from the reference program's by a relative error of at most 0.0003.
Values sent between devices are 32-bit elements; how exact they have to be, the bound alone decides.
A program may use at most 64 MiB of HBM per device.

```python
import math
import jax
import jax.numpy as jnp
from jax import lax

PATCH = 128
NCOLS = 2048
ROWS_DEV = 16
POS_DEV = 4
NROWS = 1024
SLICES = 8
POSITIONS = 256


def draw_object_field(key, part):
    layer_shape = (SLICES, NROWS, NCOLS)
    key_real, key_imag = jax.random.split(jax.random.fold_in(key, 11))
    real_part = jax.random.uniform(key_real, layer_shape, jnp.float32, 0.8, 1.2)
    imag_part = jax.random.uniform(key_imag, layer_shape, jnp.float32, -0.25, 0.25)
    return jnp.stack([real_part, imag_part], axis=0)


def draw_positions(key, part):
    key_rows, key_cols = jax.random.split(jax.random.fold_in(key, 23))
    owner_strip = jnp.arange(POSITIONS, dtype=jnp.int32) // POS_DEV
    row_offsets = owner_strip * ROWS_DEV + jax.random.randint(key_rows, (POSITIONS,), 0, ROWS_DEV, dtype=jnp.int32)
    col_offsets = jax.random.randint(key_cols, (POSITIONS,), 0, NCOLS, dtype=jnp.int32)
    return jnp.stack([row_offsets, col_offsets], axis=1)


def block_levels(own_key, shape, shards, low, high):
    factor_of, own = 1.0, jax.random.fold_in(own_key, 6)
    for position, parts in shards:
        draws = jnp.exp(jax.random.uniform(jax.random.fold_in(own, position), (parts,), jnp.float32, low / len(shards), high / len(shards)))
        factor_of = factor_of * jnp.repeat(draws, shape[position] // parts).reshape([-1 if axis == position else 1 for axis in range(len(shape))])
    return factor_of


def bell_draw(own_key, shape, deviation, bound, cuts=(), kind=jnp.bfloat16):
    factor_of = block_levels(own_key, shape, cuts, -0.22, 0.18) if cuts else 1.0
    values = jax.random.normal(own_key, shape, jnp.float32) * deviation * factor_of
    return jnp.minimum(jnp.maximum(values, -bound), bound).astype(kind)


def setup_inputs(seed: int = 0) -> dict:
    arg_keys = jax.random.split(jax.random.key(seed), 8)
    object_field = draw_object_field(jax.random.fold_in(arg_keys[7], 71), 0)
    first_moment = bell_draw(arg_keys[1], (2, SLICES, NROWS, NCOLS), 0.3, 1.8, ((1, 4), (2, 64)), jnp.float32)
    second_moment = jnp.clip(jnp.exp(math.log(0.1) - 4.6051702 * jax.random.uniform(arg_keys[2], (2, SLICES, NROWS, NCOLS), jnp.float32) ** block_levels(arg_keys[2], (2, SLICES, NROWS, NCOLS), ((1, 4), (2, 64)), -0.2, 0.2)), 0.001, 0.1)
    probe_wave = bell_draw(arg_keys[3], (2, PATCH, PATCH), 1.0, 6.0, (), jnp.float32)
    measured = jnp.clip(4.0 * jax.random.uniform(arg_keys[4], (POSITIONS, PATCH, PATCH), jnp.float32) ** block_levels(arg_keys[4], (POSITIONS, PATCH, PATCH), ((0, 64),), -0.2, 0.2), 0.0, 4.0)
    positions = draw_positions(jax.random.fold_in(arg_keys[7], 71), 0)
    fresnel = jnp.clip(jnp.exp(jax.random.uniform(arg_keys[6], (1,), jnp.float32, math.log(0.002), math.log(0.02))), 0.002, 0.02)
    return {"object_field": object_field, "first_moment": first_moment, "second_moment": second_moment, "probe_wave": probe_wave, "measured": measured, "positions": positions, "fresnel": fresnel}


beta_one = 0.9
beta_two = 0.999
learn_rate = 0.05
adam_eps = 1e-08
adam_step = 10.0

def matmul(left, right):
    return jnp.dot(left, right, precision=lax.Precision.HIGHEST)

def dft_tables(fresnel, patch_width):
    freq_index = jnp.arange(patch_width, dtype=jnp.int32)
    product = freq_index[:, None] * freq_index[None, :] % patch_width
    phase_angle = 2.0 * jnp.pi / patch_width * product.astype(jnp.float32)
    norm_scale = 1.0 / jnp.sqrt(jnp.asarray(patch_width, jnp.float32))
    four_real = jnp.cos(phase_angle) * norm_scale
    four_imag = -jnp.sin(phase_angle) * norm_scale
    signed = jnp.where(freq_index < patch_width // 2, freq_index, freq_index - patch_width).astype(jnp.float32)
    fresnel_phase = fresnel[0] * signed * signed
    kernel_real = jnp.cos(fresnel_phase)
    kernel_imag = -jnp.sin(fresnel_phase)
    left_real = four_real * kernel_real[None, :] + four_imag * kernel_imag[None, :]
    left_imag = four_real * kernel_imag[None, :] - four_imag * kernel_real[None, :]
    prop_real = matmul(left_real, four_real) - matmul(left_imag, four_imag)
    prop_imag = matmul(left_real, four_imag) + matmul(left_imag, four_real)
    return (four_real, four_imag, prop_real, prop_imag)

def complex_mul(left, right):
    left_real, left_imag = (left[..., 0, :, :], left[..., 1, :, :])
    right_real, right_imag = (right[..., 0, :, :], right[..., 1, :, :])
    return jnp.stack([left_real * right_real - left_imag * right_imag, left_real * right_imag + left_imag * right_real], axis=-3)

def apply_left(mat_real, mat_imag, wave_field):
    field_real, field_imag = (wave_field[..., 0, :, :], wave_field[..., 1, :, :])
    highest = lax.Precision.HIGHEST
    out_real = jnp.einsum('jk,...kl->...jl', mat_real, field_real, precision=highest) - jnp.einsum('jk,...kl->...jl', mat_imag, field_imag, precision=highest)
    out_imag = jnp.einsum('jk,...kl->...jl', mat_real, field_imag, precision=highest) + jnp.einsum('jk,...kl->...jl', mat_imag, field_real, precision=highest)
    return jnp.stack([out_real, out_imag], axis=-3)

def apply_right(wave_field, mat_real, mat_imag):
    field_real, field_imag = (wave_field[..., 0, :, :], wave_field[..., 1, :, :])
    highest = lax.Precision.HIGHEST
    out_real = jnp.einsum('...jk,kl->...jl', field_real, mat_real, precision=highest) - jnp.einsum('...jk,kl->...jl', field_imag, mat_imag, precision=highest)
    out_imag = jnp.einsum('...jk,kl->...jl', field_real, mat_imag, precision=highest) + jnp.einsum('...jk,kl->...jl', field_imag, mat_real, precision=highest)
    return jnp.stack([out_real, out_imag], axis=-3)

def propagate(tables, wave_field):
    four_real, four_imag, prop_real, prop_imag = tables
    return apply_right(apply_left(prop_real, prop_imag, wave_field), prop_real.T, prop_imag.T)

def far_field(tables, wave_field):
    four_real, four_imag, prop_real, prop_imag = tables
    return apply_right(apply_left(four_real, four_imag, wave_field), four_real, four_imag)

def position_loss(patches, probe_wave, pattern, tables):
    wave_field = probe_wave
    for slice_index in range(patches.shape[1]):
        wave_field = propagate(tables, complex_mul(wave_field, patches[:, slice_index]))
    far_wave = far_field(tables, wave_field)
    intensity = far_wave[0] * far_wave[0] + far_wave[1] * far_wave[1]
    return 0.5 * jnp.sum((intensity - pattern) ** 2)

def adam_update(object_field, first_moment, second_moment, gradient):
    first_new = beta_one * first_moment + (1.0 - beta_one) * gradient
    second_new = beta_two * second_moment + (1.0 - beta_two) * gradient * gradient
    first_hat = first_new / (1.0 - beta_one ** adam_step)
    second_hat = second_new / (1.0 - beta_two ** adam_step)
    object_new = object_field - learn_rate * first_hat / (jnp.sqrt(second_hat) + adam_eps)
    return (object_new, first_new, second_new)

def reference(object_field, first_moment, second_moment, probe_wave, measured, positions, fresnel):
    patch_width = probe_wave.shape[-1]
    tables = dft_tables(fresnel, patch_width)
    rows_total = object_field.shape[2]
    cols_total = object_field.shape[3]
    extended = jnp.concatenate([object_field, object_field[:, :, :patch_width]], axis=2)
    extended = jnp.concatenate([extended, extended[:, :, :, :patch_width]], axis=3)
    grad_fn = jax.grad(position_loss)
    zero_index = jnp.zeros((), jnp.int32)

    def one_position(gradient, inputs):
        offset, pattern = inputs
        start = (zero_index, zero_index, offset[0].astype(jnp.int32), offset[1].astype(jnp.int32))
        patches = lax.dynamic_slice(extended, start, (2, SLICES, patch_width, patch_width))
        piece = grad_fn(patches, probe_wave, pattern, tables)
        current = lax.dynamic_slice(gradient, start, (2, SLICES, patch_width, patch_width))
        return (lax.dynamic_update_slice(gradient, current + piece, start), None)
    gradient, unused = lax.scan(one_position, jnp.zeros(extended.shape, jnp.float32), (positions, measured))
    main_part = gradient[:, :, :rows_total].at[:, :, :patch_width].add(gradient[:, :, rows_total:])
    gradient = main_part[..., :cols_total].at[..., :patch_width].add(main_part[..., cols_total:])
    return adam_update(object_field, first_moment, second_moment, gradient)
```

```python
import functools

import jax
import jax.numpy as jnp
import numpy as np
from jax import lax
from jax.experimental import pallas as pl
from jax.experimental.pallas import tpu as pltpu
from jax.sharding import PartitionSpec as P

beta_one = 0.9
beta_two = 0.999
learn_rate = 0.05
adam_eps = 1e-08
adam_step = 10.0

PATCH = 128
ROWS = 16
SPAN = PATCH // ROWS
REACH = SPAN + 1
MESH = pl.DeviceIdType.MESH


def fourier_table():
    index = np.arange(PATCH)
    angle = 2.0 * np.pi / PATCH * ((index[:, None] * index[None, :]) % PATCH)
    table = np.stack([np.cos(angle), -np.sin(angle)]) / np.sqrt(PATCH)
    return jnp.asarray(table.astype(np.float32))


def split(value):
    high = value.astype(jnp.bfloat16)
    low = (value - high.astype(jnp.float32)).astype(jnp.bfloat16)
    return high, low


def rolled(value, amount, axis, bits):
    for bit in range(bits):
        taken = jnp.broadcast_to((amount >> bit) & 1, value.shape) == 1
        value = jnp.where(taken, pltpu.roll(value, 1 << bit, axis), value)
    return value


def dot(left, right):
    return jnp.dot(left, right, preferred_element_type=jnp.float32)


def both_sides(tab, left, right, real, imag):
    high, low = split(jnp.concatenate([real, imag], axis=1))
    wide = dot(jnp.concatenate([high, low], axis=0), tab[right, 0])
    fine = dot(high, tab[right, 1])
    turned = wide[:PATCH] + wide[PATCH:] + fine
    high, low = split(jnp.concatenate([turned[:, :PATCH], turned[:, PATCH:]], axis=0))
    wide = dot(tab[left, 0], jnp.concatenate([high, low], axis=1))
    fine = dot(tab[left, 1], high)
    done = wide[:, :PATCH] + wide[:, PATCH:] + fine
    return done[:PATCH], done[PATCH:]


def fill_tables(tab, four, fresnel):
    four_real, four_imag = four[0], four[1]

    def phase(axis):
        index = lax.broadcasted_iota(jnp.int32, (PATCH, PATCH), axis)
        signed = jnp.where(index < PATCH // 2, index, index - PATCH).astype(jnp.float32)
        angle = fresnel * signed * signed
        return jnp.cos(angle), -jnp.sin(angle)

    def scaled(axis):
        real, imag = phase(axis)
        return four_real * real - four_imag * imag, four_real * imag + four_imag * real

    def put(slot, real, imag, sign):
        top = jnp.concatenate([real, -imag if sign > 0 else imag], axis=1)
        bottom = jnp.concatenate([imag if sign > 0 else -imag, real], axis=1)
        high, low = split(jnp.concatenate([top, bottom], axis=0))
        tab[slot, 0] = high
        tab[slot, 1] = low

    def full(left, right):
        return jnp.dot(
            left, right, precision=lax.Precision.HIGHEST, preferred_element_type=jnp.float32
        )

    far_real, far_imag = scaled(0)
    put(2, far_real, far_imag, 1)
    prop_real = full(four_real, far_real) + full(four_imag, far_imag)
    prop_imag = full(four_real, far_imag) - full(four_imag, far_real)
    put(0, prop_real, prop_imag, 1)
    put(1, prop_real, prop_imag, -1)
    put(3, *scaled(1), -1)


def wave_kernel(
    slabs, strips, pos, fresnel, obj_in, probe_in, meas_in, four_in, out,
    obj, probe, meas, four, stage, recv, tab, saved, waves, gst,
    tile_sem, load_sem, patch_send, patch_recv, grad_send, grad_recv, own_sem,
):
    me_slab = lax.axis_index("slab")
    me_strip = lax.axis_index("strip")
    count = REACH * slabs

    def below(j):
        return lax.rem(me_strip + strips - j, strips)

    def above(j):
        return lax.rem(me_strip + j, strips)

    tiles = obj.shape[0]

    def tile_load(t):
        return pltpu.make_async_copy(
            obj_in.at[:, :, :, pl.ds(pl.multiple_of(t * PATCH, PATCH), PATCH)], obj.at[t], tile_sem.at[t]
        )

    def start_tile(t, carry):
        tile_load(t).start()
        return carry

    def wait_tile(t, carry):
        tile_load(t).wait()
        return carry

    lax.fori_loop(0, tiles, start_tile, 0)
    loads = [
        pltpu.make_async_copy(probe_in, probe, load_sem.at[0]),
        pltpu.make_async_copy(meas_in.at[me_slab], meas, load_sem.at[1]),
        pltpu.make_async_copy(four_in, four, load_sem.at[2]),
    ]
    for load in loads:
        load.start()

    barrier = pltpu.get_barrier_semaphore()

    def greet(i, carry):
        j = i // slabs
        peer = lax.rem(me_slab + lax.rem(i, slabs), slabs)

        @pl.when(i > 0)
        def _():
            pl.semaphore_signal(
                barrier, inc=1, device_id={"slab": peer, "strip": below(j)}, device_id_type=MESH
            )

        @pl.when(j > 0)
        def _():
            pl.semaphore_signal(
                barrier, inc=1, device_id={"slab": peer, "strip": above(j)}, device_id_type=MESH
            )

        return carry

    lax.fori_loop(0, count, greet, 0)
    lax.fori_loop(0, tiles, wait_tile, 0)
    lane = lax.broadcasted_iota(jnp.int32, (2, 2, ROWS, PATCH), 3)

    def cut(i, carry):
        j = i // slabs
        item = below(j) * slabs + lax.rem(i, slabs)
        column = pos[item, 1]
        tile = lax.shift_right_logical(column, 7)
        after = (tile + 1) & 15
        stage[i] = jnp.where(lane >= (column & 127), obj[tile], obj[after])
        return carry

    lax.fori_loop(0, count, cut, 0)
    pl.semaphore_wait(barrier, 2 * count - slabs - 1)

    def patch_copy(i):
        j = i // slabs
        peer = lax.rem(me_slab + lax.rem(i, slabs), slabs)
        return pltpu.make_async_remote_copy(
            src_ref=stage.at[j * slabs + peer],
            dst_ref=recv.at[me_slab, j],
            send_sem=patch_send.at[i],
            recv_sem=patch_recv.at[me_slab, j],
            device_id={"slab": peer, "strip": below(j)},
            device_id_type=MESH,
        )

    def send_patch(i, carry):
        patch_copy(i).start()
        return carry

    lax.fori_loop(1, count, send_patch, 0)
    recv[me_slab, 0] = stage[me_slab]

    for load in loads:
        load.wait()
    fill_tables(tab, four, fresnel[0])
    own = me_strip * slabs + me_slab
    own_row = pos[own, 0] - me_strip * ROWS
    own_shift = pos[own, 1] & 127
    for part in range(2):
        waves[part] = rolled(rolled(probe[part], own_row, 0, 4), own_shift, 1, 7)
    row = lax.broadcasted_iota(jnp.int32, (ROWS, PATCH), 0)

    def arrived(q):
        def one(j, carry):
            @pl.when((q != me_slab) | (j > 0))
            def _():
                pltpu.make_async_remote_copy(
                    src_ref=stage.at[0],
                    dst_ref=recv.at[q, j],
                    send_sem=patch_send.at[0],
                    recv_sem=patch_recv.at[q, j],
                    device_id={"slab": q, "strip": above(j)},
                    device_id_type=MESH,
                ).wait_recv()

            return carry

        lax.fori_loop(0, REACH, one, 0)

    def layer(s):
        q, n = s // 2, lax.rem(s, 2)
        parts = []
        for part in range(2):
            first = jnp.where(row >= own_row, recv[q, 0, part, n], recv[q, SPAN, part, n])
            rest = [recv[q, j, part, n] for j in range(1, SPAN)]
            parts.append(jnp.concatenate([first] + rest, axis=0))
        return parts

    def enter(s):
        real, imag = waves[0], waves[1]
        saved[s, 0] = real
        saved[s, 1] = imag
        layer_real, layer_imag = layer(s)
        return (
            real * layer_real - imag * layer_imag,
            real * layer_imag + imag * layer_real,
        )

    def forward(s, carry):
        @pl.when(lax.rem(s, 2) == 0)
        def _():
            arrived(s // 2)

        real, imag = both_sides(tab, 0, 1, *enter(s))
        waves[0] = real
        waves[1] = imag
        return carry

    slices = 2 * slabs
    lax.fori_loop(0, slices - 1, forward, 0)
    real, imag = both_sides(tab, 2, 3, *enter(slices - 1))
    factor = 2.0 * (real * real + imag * imag - meas[...])
    real, imag = both_sides(tab, 3, 2, real * factor, imag * factor)
    waves[0] = real
    waves[1] = imag

    def leave(s):
        q, n = s // 2, lax.rem(s, 2)
        real, imag = waves[0], waves[1]
        old_real, old_imag = saved[s, 0], saved[s, 1]
        grad_real = old_real * real + old_imag * imag
        grad_imag = old_real * imag - old_imag * real
        for j in range(SPAN):
            gst[q, j, 0, n] = grad_real[j * ROWS : (j + 1) * ROWS]
            gst[q, j, 1, n] = grad_imag[j * ROWS : (j + 1) * ROWS]

    def grad_copy(q, j):
        return pltpu.make_async_remote_copy(
            src_ref=gst.at[q, lax.rem(j, SPAN)],
            dst_ref=out.at[j, me_slab],
            send_sem=grad_send.at[q, j],
            recv_sem=grad_recv.at[j, me_slab],
            device_id={"slab": q, "strip": above(j)},
            device_id_type=MESH,
        )

    own_copy = pltpu.make_async_copy(gst.at[me_slab, 0], out.at[0, me_slab], own_sem)

    def send_grads(q):
        def one(j, carry):
            @pl.when((q != me_slab) | (j > 0))
            def _():
                grad_copy(q, j).start()

            return carry

        lax.fori_loop(0, REACH, one, 0)

        @pl.when(q == me_slab)
        def _():
            own_copy.start()

    def backward(i, carry):
        s = slices - 1 - i
        leave(s)

        @pl.when(lax.rem(s, 2) == 0)
        def _():
            send_grads(s // 2)

        real, imag = waves[0], waves[1]
        layer_real, layer_imag = layer(s)
        real, imag = both_sides(
            tab, 1, 0,
            layer_real * real + layer_imag * imag,
            layer_real * imag - layer_imag * real,
        )
        waves[0] = real
        waves[1] = imag
        return carry

    lax.fori_loop(0, slices - 1, backward, 0)
    leave(0)
    send_grads(0)

    def finish_patch(i, carry):
        patch_copy(i).wait_send()
        return carry

    lax.fori_loop(1, count, finish_patch, 0)

    def finish_grad(i, carry):
        j, q = i // slabs, lax.rem(i, slabs)

        @pl.when((q != me_slab) | (j > 0))
        def _():
            grad_copy(q, j).wait_send()
            pltpu.make_async_remote_copy(
                src_ref=gst.at[q, 0],
                dst_ref=out.at[j, q],
                send_sem=grad_send.at[q, j],
                recv_sem=grad_recv.at[j, q],
                device_id={"slab": q, "strip": below(j)},
                device_id_type=MESH,
            ).wait_recv()

        return carry

    lax.fori_loop(0, count, finish_grad, 0)
    own_copy.wait()


def update_kernel(slabs, strips, pos, pieces, obj, first, second, obj_out, first_out, second_out, grad):
    me_strip = lax.axis_index("strip")
    grad[...] = jnp.zeros_like(grad)
    shape = (2, 2, ROWS, PATCH)
    lane = lax.broadcasted_iota(jnp.int32, shape, 3)
    row = lax.broadcasted_iota(jnp.int32, shape, 2)

    def place(i, carry):
        j, k = i // slabs, lax.rem(i, slabs)
        owner = lax.rem(me_strip + strips - j, strips)
        item = owner * slabs + k
        column = pos[item, 1]
        local_row = pos[item, 0] - owner * ROWS
        low = jnp.where(j == 0, local_row, 0)
        high = jnp.where(j == SPAN, local_row, ROWS)
        tile = lax.shift_right_logical(column, 7)
        after = (tile + 1) & 15
        shift = column & 127
        piece = jnp.where((row >= low) & (row < high), pieces[j, k], 0.0)
        here = pl.ds(pl.multiple_of(tile * PATCH, PATCH), PATCH)
        there = pl.ds(pl.multiple_of(after * PATCH, PATCH), PATCH)
        grad[:, :, :, here] += jnp.where(lane >= shift, piece, 0.0)
        grad[:, :, :, there] += jnp.where(lane >= shift, 0.0, piece)
        return carry

    lax.fori_loop(0, REACH * slabs, place, 0)
    gradient = grad[...]
    first_new = beta_one * first[...] + (1.0 - beta_one) * gradient
    second_new = beta_two * second[...] + (1.0 - beta_two) * gradient * gradient
    first_hat = first_new / (1.0 - beta_one**adam_step)
    second_hat = second_new / (1.0 - beta_two**adam_step)
    obj_out[...] = obj[...] - learn_rate * first_hat / (jnp.sqrt(second_hat) + adam_eps)
    first_out[...] = first_new
    second_out[...] = second_new


def shards(slabs, strips, object_field, first_moment, second_moment, probe_wave, measured, positions, fresnel):
    vmem = pl.BlockSpec(memory_space=pltpu.VMEM)
    smem = pl.BlockSpec(memory_space=pltpu.SMEM)
    anywhere = pl.BlockSpec(memory_space=pl.ANY)
    f32 = jnp.float32
    count = REACH * slabs
    tiles = object_field.shape[3] // PATCH
    piece = (2, 2, ROWS, PATCH)
    pair = (2, PATCH, PATCH)
    pieces = pl.pallas_call(
        functools.partial(wave_kernel, slabs, strips),
        out_shape=jax.ShapeDtypeStruct((REACH, slabs) + piece, f32),
        in_specs=[smem, smem, anywhere, anywhere, anywhere, anywhere],
        out_specs=anywhere,
        scratch_shapes=[
            pltpu.VMEM((tiles,) + piece, f32),
            pltpu.VMEM(pair, f32),
            pltpu.VMEM((PATCH, PATCH), f32),
            pltpu.VMEM(pair, f32),
            pltpu.VMEM((count,) + piece, f32),
            pltpu.VMEM((slabs, REACH) + piece, f32),
            pltpu.VMEM((4, 2, 2 * PATCH, 2 * PATCH), jnp.bfloat16),
            pltpu.VMEM((2 * slabs,) + pair, f32),
            pltpu.VMEM(pair, f32),
            pltpu.VMEM((slabs, SPAN) + piece, f32),
            pltpu.SemaphoreType.DMA((tiles,)),
            pltpu.SemaphoreType.DMA((3,)),
            pltpu.SemaphoreType.DMA((count,)),
            pltpu.SemaphoreType.DMA((slabs, REACH)),
            pltpu.SemaphoreType.DMA((slabs, REACH)),
            pltpu.SemaphoreType.DMA((REACH, slabs)),
            pltpu.SemaphoreType.DMA(()),
        ],
        compiler_params=pltpu.CompilerParams(collective_id=0, has_side_effects=True),
    )(positions, fresnel, object_field, probe_wave, measured, fourier_table())
    like = jax.ShapeDtypeStruct(object_field.shape, f32)
    return pl.pallas_call(
        functools.partial(update_kernel, slabs, strips),
        out_shape=(like, like, like),
        in_specs=[smem, vmem, vmem, vmem, vmem],
        out_specs=(vmem, vmem, vmem),
        scratch_shapes=[pltpu.VMEM(object_field.shape, f32)],
    )(positions, pieces, object_field, first_moment, second_moment)


def solution(mesh):
    spec = P(None, "slab", "strip", None)
    return jax.shard_map(
        functools.partial(shards, mesh.shape["slab"], mesh.shape["strip"]),
        mesh=mesh,
        in_specs=(spec, spec, spec, P(), P("strip", None, None), P(), P()),
        out_specs=(spec, spec, spec),
        check_vma=False,
    )
```

```python
import functools

import jax
import jax.numpy as jnp
import numpy as np
from jax import lax
from jax.experimental import pallas as pl
from jax.experimental.pallas import tpu as pltpu
from jax.sharding import PartitionSpec as P

beta_one = 0.9
beta_two = 0.999
learn_rate = 0.05
adam_eps = 1e-08
adam_step = 10.0

PATCH = 128
ROWS = 16
SPAN = PATCH // ROWS
REACH = SPAN + 1
CENTER = 4
MESH = pl.DeviceIdType.MESH


def fourier_table():
    index = np.arange(PATCH)
    angle = 2.0 * np.pi / PATCH * ((index[:, None] * index[None, :]) % PATCH)
    table = np.stack([np.cos(angle), -np.sin(angle)]) / np.sqrt(PATCH)
    return jnp.asarray(table.astype(np.float32))


def split(value):
    high = value.astype(jnp.bfloat16)
    low = (value - high.astype(jnp.float32)).astype(jnp.bfloat16)
    return high, low


def rolled(value, amount, axis, bits):
    for bit in range(bits):
        taken = jnp.broadcast_to((amount >> bit) & 1, value.shape) == 1
        value = jnp.where(taken, pltpu.roll(value, 1 << bit, axis), value)
    return value


def dot(left, right):
    return jnp.dot(left, right, preferred_element_type=jnp.float32)


def both_sides(tab, left, right, real, imag):
    high, low = split(jnp.concatenate([real, imag], axis=1))
    wide = dot(jnp.concatenate([high, low], axis=0), tab[right, 0])
    fine = dot(high, tab[right, 1])
    turned = wide[:PATCH] + wide[PATCH:] + fine
    high, low = split(jnp.concatenate([turned[:, :PATCH], turned[:, PATCH:]], axis=0))
    wide = dot(tab[left, 0], jnp.concatenate([high, low], axis=1))
    fine = dot(tab[left, 1], high)
    done = wide[:, :PATCH] + wide[:, PATCH:] + fine
    return done[:PATCH], done[PATCH:]


def fill_tables(tab, four, fresnel):
    four_real, four_imag = four[0], four[1]

    def phase(axis):
        index = lax.broadcasted_iota(jnp.int32, (PATCH, PATCH), axis)
        signed = jnp.where(index < PATCH // 2, index, index - PATCH).astype(jnp.float32)
        angle = fresnel * signed * signed
        return jnp.cos(angle), -jnp.sin(angle)

    def scaled(axis):
        real, imag = phase(axis)
        return four_real * real - four_imag * imag, four_real * imag + four_imag * real

    def put(slot, real, imag, sign):
        top = jnp.concatenate([real, -imag if sign > 0 else imag], axis=1)
        bottom = jnp.concatenate([imag if sign > 0 else -imag, real], axis=1)
        high, low = split(jnp.concatenate([top, bottom], axis=0))
        tab[slot, 0] = high
        tab[slot, 1] = low

    def full(left, right):
        return jnp.dot(
            left, right, precision=lax.Precision.HIGHEST, preferred_element_type=jnp.float32
        )

    far_real, far_imag = scaled(0)
    put(2, far_real, far_imag, 1)
    prop_real = full(four_real, far_real) + full(four_imag, far_imag)
    prop_imag = full(four_real, far_imag) - full(four_imag, far_real)
    put(0, prop_real, prop_imag, 1)
    put(1, prop_real, prop_imag, -1)
    put(3, *scaled(1), -1)


def wave_kernel(
    slabs, strips, pos_in, fresnel_in, obj_in, probe_in, meas_in, four_in, out,
    pos, fresnel, obj, probe, meas, four, stage, recv, tab, saved, waves, gst,
    tile_sem, load_sem, meas_sem, patch_send, patch_recv, grad_send, grad_recv, own_sem,
):
    me_slab = lax.axis_index("slab")
    me_strip = lax.axis_index("strip")
    count = REACH * slabs

    def below(j):
        return lax.rem(me_strip + strips + CENTER - j, strips)

    def above(j):
        return lax.rem(me_strip + strips - CENTER + j, strips)

    def remote(peer, j):
        return (peer != me_slab) | (j != CENTER)

    tiles = obj.shape[0]

    def tile_load(t):
        return pltpu.make_async_copy(
            obj_in.at[:, :, :, pl.ds(pl.multiple_of(t * PATCH, PATCH), PATCH)], obj.at[t], tile_sem.at[t]
        )

    def start_tile(t, carry):
        tile_load(t).start()
        return carry

    def wait_tile(t, carry):
        tile_load(t).wait()
        return carry

    pos_load = pltpu.make_async_copy(pos_in, pos, load_sem.at[2])
    pos_load.start()
    lax.fori_loop(0, tiles, start_tile, 0)
    loads = [
        pltpu.make_async_copy(probe_in, probe, load_sem.at[0]),
        pltpu.make_async_copy(four_in, four, load_sem.at[1]),
        pltpu.make_async_copy(fresnel_in, fresnel, load_sem.at[3]),
    ]
    for load in loads:
        load.start()

    barrier = pltpu.get_barrier_semaphore()

    def greet(i, carry):
        j = i // slabs
        peer = lax.rem(i, slabs)

        @pl.when(remote(peer, j))
        def _():
            pl.semaphore_signal(
                barrier, inc=1, device_id={"slab": peer, "strip": below(j)}, device_id_type=MESH
            )

        return carry

    lax.fori_loop(0, count, greet, 0)
    pos_load.wait()
    lax.fori_loop(0, tiles, wait_tile, 0)
    lane = lax.broadcasted_iota(jnp.int32, (2, 2, ROWS, PATCH), 3)

    def cut(i, carry):
        j = i // slabs
        item = lax.rem(me_strip + strips - j, strips) * slabs + lax.rem(i, slabs)
        column = pos[1, item]
        tile = lax.shift_right_logical(column, 7)
        after = (tile + 1) & 15
        stage[i] = jnp.where(lane >= (column & 127), obj[tile], obj[after])
        return carry

    lax.fori_loop(0, count, cut, 0)
    pl.semaphore_wait(barrier, count - 1)

    def patch_copy(j, peer):
        return pltpu.make_async_remote_copy(
            src_ref=stage.at[j * slabs + peer],
            dst_ref=recv.at[me_slab, j],
            send_sem=patch_send.at[j * slabs + peer],
            recv_sem=patch_recv.at[me_slab, j],
            device_id={"slab": peer, "strip": below(j)},
            device_id_type=MESH,
        )

    def patch_order(i):
        return lax.rem(i, REACH), lax.rem(me_slab + i // REACH, slabs)

    def send_patch(i, carry):
        j, peer = patch_order(i)

        @pl.when(remote(peer, j))
        def _():
            patch_copy(j, peer).start()

        return carry

    lax.fori_loop(0, count, send_patch, 0)
    meas_copy = pltpu.make_async_remote_copy(
        src_ref=meas_in.at[me_slab],
        dst_ref=meas,
        send_sem=meas_sem.at[0],
        recv_sem=meas_sem.at[1],
        device_id={"slab": me_slab, "strip": below(0)},
        device_id_type=MESH,
    )
    meas_copy.start()
    recv[me_slab, CENTER] = stage[CENTER * slabs + me_slab]

    for load in loads:
        load.wait()
    fill_tables(tab, four, fresnel[0])
    owner = lax.rem(me_strip + strips - CENTER, strips)
    own = owner * slabs + me_slab
    own_row = pos[0, own] - owner * ROWS
    own_shift = pos[1, own] & 127
    for part in range(2):
        waves[part] = rolled(rolled(probe[part], own_row, 0, 4), own_shift, 1, 7)
    row = lax.broadcasted_iota(jnp.int32, (ROWS, PATCH), 0)

    def arrived(q):
        def one(j, carry):
            @pl.when(remote(q, j))
            def _():
                pltpu.make_async_remote_copy(
                    src_ref=stage.at[0],
                    dst_ref=recv.at[q, j],
                    send_sem=patch_send.at[0],
                    recv_sem=patch_recv.at[q, j],
                    device_id={"slab": q, "strip": above(j)},
                    device_id_type=MESH,
                ).wait_recv()

            return carry

        lax.fori_loop(0, REACH, one, 0)

    def layer(s):
        q, n = s // 2, lax.rem(s, 2)
        parts = []
        for part in range(2):
            first = jnp.where(row >= own_row, recv[q, 0, part, n], recv[q, SPAN, part, n])
            rest = [recv[q, j, part, n] for j in range(1, SPAN)]
            parts.append(jnp.concatenate([first] + rest, axis=0))
        return parts

    def enter(s):
        real, imag = waves[0], waves[1]
        saved[s, 0] = real
        saved[s, 1] = imag
        layer_real, layer_imag = layer(s)
        return (
            real * layer_real - imag * layer_imag,
            real * layer_imag + imag * layer_real,
        )

    def forward(s, carry):
        @pl.when(lax.rem(s, 2) == 0)
        def _():
            arrived(s // 2)

        real, imag = both_sides(tab, 0, 1, *enter(s))
        waves[0] = real
        waves[1] = imag
        return carry

    slices = 2 * slabs
    lax.fori_loop(0, slices - 1, forward, 0)
    real, imag = both_sides(tab, 2, 3, *enter(slices - 1))
    meas_copy.wait_recv()
    factor = 2.0 * (real * real + imag * imag - meas[...])
    real, imag = both_sides(tab, 3, 2, real * factor, imag * factor)
    waves[0] = real
    waves[1] = imag

    def leave(s):
        q, n = s // 2, lax.rem(s, 2)
        real, imag = waves[0], waves[1]
        old_real, old_imag = saved[s, 0], saved[s, 1]
        grad_real = old_real * real + old_imag * imag
        grad_imag = old_real * imag - old_imag * real
        for j in range(SPAN):
            gst[q, j, 0, n] = grad_real[j * ROWS : (j + 1) * ROWS]
            gst[q, j, 1, n] = grad_imag[j * ROWS : (j + 1) * ROWS]

    def grad_copy(q, j):
        return pltpu.make_async_remote_copy(
            src_ref=gst.at[q, lax.rem(j, SPAN)],
            dst_ref=out.at[j, me_slab],
            send_sem=grad_send.at[q, j],
            recv_sem=grad_recv.at[j, me_slab],
            device_id={"slab": q, "strip": above(j)},
            device_id_type=MESH,
        )

    own_copy = pltpu.make_async_copy(gst.at[me_slab, CENTER], out.at[CENTER, me_slab], own_sem)

    def send_grads(q):
        def one(j, carry):
            @pl.when(remote(q, j))
            def _():
                grad_copy(q, j).start()

            return carry

        lax.fori_loop(0, REACH, one, 0)

        @pl.when(q == me_slab)
        def _():
            own_copy.start()

    def backward(i, carry):
        s = slices - 1 - i
        leave(s)

        @pl.when(lax.rem(s, 2) == 0)
        def _():
            send_grads(s // 2)

        real, imag = waves[0], waves[1]
        layer_real, layer_imag = layer(s)
        real, imag = both_sides(
            tab, 1, 0,
            layer_real * real + layer_imag * imag,
            layer_real * imag - layer_imag * real,
        )
        waves[0] = real
        waves[1] = imag
        return carry

    lax.fori_loop(0, slices - 1, backward, 0)
    leave(0)
    send_grads(0)

    def finish_patch(i, carry):
        j, peer = patch_order(i)

        @pl.when(remote(peer, j))
        def _():
            patch_copy(j, peer).wait_send()

        return carry

    lax.fori_loop(0, count, finish_patch, 0)
    meas_copy.wait_send()

    def finish_grad(i, carry):
        j, q = i // slabs, lax.rem(i, slabs)

        @pl.when(remote(q, j))
        def _():
            grad_copy(q, j).wait_send()
            pltpu.make_async_remote_copy(
                src_ref=gst.at[q, 0],
                dst_ref=out.at[j, q],
                send_sem=grad_send.at[q, j],
                recv_sem=grad_recv.at[j, q],
                device_id={"slab": q, "strip": below(j)},
                device_id_type=MESH,
            ).wait_recv()

        return carry

    lax.fori_loop(0, count, finish_grad, 0)
    own_copy.wait()


def update_kernel(slabs, strips, pos, pieces, obj, first, second, obj_out, first_out, second_out, grad):
    me_strip = lax.axis_index("strip")
    grad[...] = jnp.zeros_like(grad)
    shape = (2, 2, ROWS, PATCH)
    lane = lax.broadcasted_iota(jnp.int32, shape, 3)
    row = lax.broadcasted_iota(jnp.int32, shape, 2)

    def place(i, carry):
        j, k = i // slabs, lax.rem(i, slabs)
        owner = lax.rem(me_strip + strips - j, strips)
        item = owner * slabs + k
        column = pos[1, item]
        local_row = pos[0, item] - owner * ROWS
        low = jnp.where(j == 0, local_row, 0)
        high = jnp.where(j == SPAN, local_row, ROWS)
        tile = lax.shift_right_logical(column, 7)
        after = (tile + 1) & 15
        shift = column & 127
        piece = jnp.where((row >= low) & (row < high), pieces[j, k], 0.0)
        here = pl.ds(pl.multiple_of(tile * PATCH, PATCH), PATCH)
        there = pl.ds(pl.multiple_of(after * PATCH, PATCH), PATCH)
        grad[:, :, :, here] += jnp.where(lane >= shift, piece, 0.0)
        grad[:, :, :, there] += jnp.where(lane >= shift, 0.0, piece)
        return carry

    lax.fori_loop(0, REACH * slabs, place, 0)
    gradient = grad[...]
    first_new = beta_one * first[...] + (1.0 - beta_one) * gradient
    second_new = beta_two * second[...] + (1.0 - beta_two) * gradient * gradient
    first_hat = first_new / (1.0 - beta_one**adam_step)
    second_hat = second_new / (1.0 - beta_two**adam_step)
    obj_out[...] = obj[...] - learn_rate * first_hat / (jnp.sqrt(second_hat) + adam_eps)
    first_out[...] = first_new
    second_out[...] = second_new


def shards(slabs, strips, object_field, first_moment, second_moment, probe_wave, measured, positions, fresnel):
    vmem = pl.BlockSpec(memory_space=pltpu.VMEM)
    smem = pl.BlockSpec(memory_space=pltpu.SMEM)
    anywhere = pl.BlockSpec(memory_space=pl.ANY)
    f32 = jnp.float32
    count = REACH * slabs
    tiles = object_field.shape[3] // PATCH
    piece = (2, 2, ROWS, PATCH)
    pair = (2, PATCH, PATCH)
    turned = positions.T
    pieces = pl.pallas_call(
        functools.partial(wave_kernel, slabs, strips),
        out_shape=jax.ShapeDtypeStruct((REACH, slabs) + piece, f32),
        in_specs=[pl.BlockSpec(memory_space=pltpu.HBM)] * 6,
        out_specs=anywhere,
        scratch_shapes=[
            pltpu.SMEM((2, positions.shape[0]), jnp.int32),
            pltpu.SMEM((1,), f32),
            pltpu.VMEM((tiles,) + piece, f32),
            pltpu.VMEM(pair, f32),
            pltpu.VMEM((PATCH, PATCH), f32),
            pltpu.VMEM(pair, f32),
            pltpu.VMEM((count,) + piece, f32),
            pltpu.VMEM((slabs, REACH) + piece, f32),
            pltpu.VMEM((4, 2, 2 * PATCH, 2 * PATCH), jnp.bfloat16),
            pltpu.VMEM((2 * slabs,) + pair, f32),
            pltpu.VMEM(pair, f32),
            pltpu.VMEM((slabs, SPAN) + piece, f32),
            pltpu.SemaphoreType.DMA((tiles,)),
            pltpu.SemaphoreType.DMA((4,)),
            pltpu.SemaphoreType.DMA((2,)),
            pltpu.SemaphoreType.DMA((count,)),
            pltpu.SemaphoreType.DMA((slabs, REACH)),
            pltpu.SemaphoreType.DMA((slabs, REACH)),
            pltpu.SemaphoreType.DMA((REACH, slabs)),
            pltpu.SemaphoreType.DMA(()),
        ],
        compiler_params=pltpu.CompilerParams(
            collective_id=0, has_side_effects=True, vmem_limit_bytes=62 << 20
        ),
    )(turned, fresnel, object_field, probe_wave, measured, fourier_table())
    like = jax.ShapeDtypeStruct(object_field.shape, f32)
    return pl.pallas_call(
        functools.partial(update_kernel, slabs, strips),
        out_shape=(like, like, like),
        in_specs=[smem, vmem, vmem, vmem, vmem],
        out_specs=(vmem, vmem, vmem),
        scratch_shapes=[pltpu.VMEM(object_field.shape, f32)],
        compiler_params=pltpu.CompilerParams(vmem_limit_bytes=12 << 20),
    )(turned, pieces, object_field, first_moment, second_moment)


def solution(mesh):
    spec = P(None, "slab", "strip", None)
    return jax.shard_map(
        functools.partial(shards, mesh.shape["slab"], mesh.shape["strip"]),
        mesh=mesh,
        in_specs=(spec, spec, spec, P(), P("strip", None, None), P(), P()),
        out_specs=(spec, spec, spec),
        check_vma=False,
    )
```

```python
import functools

import jax
import jax.numpy as jnp
import numpy as np
from jax import lax
from jax.experimental import pallas as pl
from jax.experimental.pallas import tpu as pltpu
from jax.sharding import PartitionSpec as P

beta_one = 0.9
beta_two = 0.999
learn_rate = 0.05
adam_eps = 1e-08
adam_step = 10.0

PATCH = 128
ROWS = 16
SPAN = PATCH // ROWS
REACH = SPAN + 1
CENTER = SPAN // 2
AHEAD = 6
MESH = pl.DeviceIdType.MESH


def fourier_table():
    index = np.arange(PATCH)
    angle = 2.0 * np.pi / PATCH * ((index[:, None] * index[None, :]) % PATCH)
    table = np.stack([np.cos(angle), -np.sin(angle)]) / np.sqrt(PATCH)
    return jnp.asarray(table.astype(np.float32))


def split(value):
    high = value.astype(jnp.bfloat16)
    low = (value - high.astype(jnp.float32)).astype(jnp.bfloat16)
    return high, low


def rolled(value, amount, axis, bits):
    for bit in range(bits):
        taken = jnp.broadcast_to((amount >> bit) & 1, value.shape) == 1
        value = jnp.where(taken, pltpu.roll(value, 1 << bit, axis), value)
    return value


def dot(left, right):
    return jnp.dot(left, right, preferred_element_type=jnp.float32)


def both_sides(tab, left, right, real, imag):
    high, low = split(jnp.concatenate([real, imag], axis=1))
    wide = dot(jnp.concatenate([high, low], axis=0), tab[right, 0])
    fine = dot(high, tab[right, 1])
    turned = wide[:PATCH] + wide[PATCH:] + fine
    high, low = split(jnp.concatenate([turned[:, :PATCH], turned[:, PATCH:]], axis=0))
    wide = dot(tab[left, 0], jnp.concatenate([high, low], axis=1))
    fine = dot(tab[left, 1], high)
    done = wide[:, :PATCH] + wide[:, PATCH:] + fine
    return done[:PATCH], done[PATCH:]


def fill_tables(tab, four, fresnel):
    four_real, four_imag = four[0], four[1]

    def phase(axis):
        index = lax.broadcasted_iota(jnp.int32, (PATCH, PATCH), axis)
        signed = jnp.where(index < PATCH // 2, index, index - PATCH).astype(jnp.float32)
        angle = fresnel * signed * signed
        return jnp.cos(angle), -jnp.sin(angle)

    def scaled(axis):
        real, imag = phase(axis)
        return four_real * real - four_imag * imag, four_real * imag + four_imag * real

    def put(slot, real, imag, sign):
        top = jnp.concatenate([real, -imag if sign > 0 else imag], axis=1)
        bottom = jnp.concatenate([imag if sign > 0 else -imag, real], axis=1)
        high, low = split(jnp.concatenate([top, bottom], axis=0))
        tab[slot, 0] = high
        tab[slot, 1] = low

    def full(left, right):
        return jnp.dot(
            left, right, precision=lax.Precision.HIGHEST, preferred_element_type=jnp.float32
        )

    far_real, far_imag = scaled(0)
    put(2, far_real, far_imag, 1)
    prop_real = full(four_real, far_real) + full(four_imag, far_imag)
    prop_imag = full(four_real, far_imag) - full(four_imag, far_real)
    put(0, prop_real, prop_imag, 1)
    put(1, prop_real, prop_imag, -1)
    put(3, *scaled(1), -1)


def wave_kernel(
    slabs, strips, pos_in, fresnel_in, obj_in, probe_in, meas_in, four_in, out,
    pos, fresnel, obj, probe, meas, four, stage, recv, tab, saved, waves, gst,
    tile_sem, load_sem, meas_sem, patch_send, patch_recv, grad_send, grad_recv, own_sem,
):
    me_slab = lax.axis_index("slab")
    me_strip = lax.axis_index("strip")
    count = REACH * slabs

    def moved(by):
        return lax.rem(me_strip + strips + by, strips)

    def worker(peer, j):
        return {"slab": peer, "strip": moved(CENTER - j)}

    def holder(peer, j):
        return {"slab": peer, "strip": moved(j - CENTER)}

    def remote(peer, j):
        return (peer != me_slab) | (j != CENTER)

    tiles = obj.shape[0]

    def tile_load(t):
        return pltpu.make_async_copy(
            obj_in.at[:, :, :, pl.ds(pl.multiple_of(t * PATCH, PATCH), PATCH)], obj.at[t], tile_sem.at[t]
        )

    def start_tile(t, carry):
        tile_load(t).start()
        return carry

    def wait_tile(t, carry):
        tile_load(t).wait()
        return carry

    pos_load = pltpu.make_async_copy(pos_in, pos, load_sem.at[2])
    pos_load.start()
    lax.fori_loop(0, tiles, start_tile, 0)
    loads = [
        pltpu.make_async_copy(probe_in, probe, load_sem.at[0]),
        pltpu.make_async_copy(four_in, four, load_sem.at[1]),
        pltpu.make_async_copy(fresnel_in, fresnel, load_sem.at[3]),
    ]
    for load in loads:
        load.start()

    barrier = pltpu.get_barrier_semaphore()

    def greet(i, carry):
        j, peer = i // slabs, lax.rem(i, slabs)

        @pl.when(remote(peer, j))
        def _():
            pl.semaphore_signal(
                barrier, inc=1, device_id=worker(peer, j), device_id_type=MESH
            )

        return carry

    lax.fori_loop(0, count, greet, 0)
    pos_load.wait()
    lax.fori_loop(0, tiles, wait_tile, 0)
    lane = lax.broadcasted_iota(jnp.int32, (2, 2, ROWS, PATCH), 3)

    def patch_order(i):
        return lax.rem(i, REACH), lax.rem(me_slab + i // REACH, slabs)

    def cut(i):
        j, peer = patch_order(i)
        item = moved(-j) * slabs + peer
        column = pos[1, item]
        tile = lax.shift_right_logical(column, 7)
        after = (tile + 1) & 15
        stage[j * slabs + peer] = jnp.where(lane >= (column & 127), obj[tile], obj[after])

    def cut_more(i, carry):
        cut(i)
        return carry

    def patch_copy(j, peer):
        return pltpu.make_async_remote_copy(
            src_ref=stage.at[j * slabs + peer],
            dst_ref=recv.at[me_slab, j],
            send_sem=patch_send.at[j * slabs + peer],
            recv_sem=patch_recv.at[me_slab, j],
            device_id=worker(peer, j),
            device_id_type=MESH,
        )

    def send_patch(i, carry):
        j, peer = patch_order(i)

        @pl.when(remote(peer, j))
        def _():
            patch_copy(j, peer).start()

        return carry

    lax.fori_loop(0, AHEAD, cut_more, 0)
    pl.semaphore_wait(barrier, count - 1)

    def cut_and_send(i, carry):
        send_patch(i, carry)
        cut(i + AHEAD)
        return carry

    lax.fori_loop(0, count - AHEAD, cut_and_send, 0)
    lax.fori_loop(count - AHEAD, count, send_patch, 0)
    far_meas = pltpu.make_async_remote_copy(
        src_ref=meas_in.at[me_slab],
        dst_ref=meas,
        send_sem=meas_sem.at[0],
        recv_sem=meas_sem.at[1],
        device_id={"slab": me_slab, "strip": moved(CENTER)},
        device_id_type=MESH,
    )
    far_meas.start()
    recv[me_slab, CENTER] = stage[CENTER * slabs + me_slab]

    for load in loads:
        load.wait()
    fill_tables(tab, four, fresnel[0])
    owner = moved(-CENTER)
    own = owner * slabs + me_slab
    own_row = pos[0, own] - owner * ROWS
    own_shift = pos[1, own] & 127
    for part in range(2):
        waves[part] = rolled(rolled(probe[part], own_row, 0, 4), own_shift, 1, 7)
    row = lax.broadcasted_iota(jnp.int32, (ROWS, PATCH), 0)

    def arrived(q):
        def one(j, carry):
            @pl.when(remote(q, j))
            def _():
                pltpu.make_async_remote_copy(
                    src_ref=stage.at[0],
                    dst_ref=recv.at[q, j],
                    send_sem=patch_send.at[0],
                    recv_sem=patch_recv.at[q, j],
                    device_id=holder(q, j),
                    device_id_type=MESH,
                ).wait_recv()

            return carry

        lax.fori_loop(0, REACH, one, 0)

    def layer(s):
        q, n = s // 2, lax.rem(s, 2)
        parts = []
        for part in range(2):
            first = jnp.where(row >= own_row, recv[q, 0, part, n], recv[q, SPAN, part, n])
            rest = [recv[q, j, part, n] for j in range(1, SPAN)]
            parts.append(jnp.concatenate([first] + rest, axis=0))
        return parts

    def enter(s):
        real, imag = waves[0], waves[1]
        saved[s, 0] = real
        saved[s, 1] = imag
        layer_real, layer_imag = layer(s)
        return (
            real * layer_real - imag * layer_imag,
            real * layer_imag + imag * layer_real,
        )

    def forward(s, carry):
        @pl.when(lax.rem(s, 2) == 0)
        def _():
            arrived(s // 2)

        real, imag = both_sides(tab, 0, 1, *enter(s))
        waves[0] = real
        waves[1] = imag
        return carry

    slices = 2 * slabs
    lax.fori_loop(0, slices - 1, forward, 0, unroll=True)
    real, imag = both_sides(tab, 2, 3, *enter(slices - 1))

    far_meas.wait_recv()
    factor = 2.0 * (real * real + imag * imag - meas[...])
    real, imag = both_sides(tab, 3, 2, real * factor, imag * factor)
    waves[0] = real
    waves[1] = imag

    def leave(s):
        q, n = s // 2, lax.rem(s, 2)
        real, imag = waves[0], waves[1]
        old_real, old_imag = saved[s, 0], saved[s, 1]
        grad_real = old_real * real + old_imag * imag
        grad_imag = old_real * imag - old_imag * real
        for j in range(SPAN):
            gst[q, j, 0, n] = grad_real[j * ROWS : (j + 1) * ROWS]
            gst[q, j, 1, n] = grad_imag[j * ROWS : (j + 1) * ROWS]

    def grad_copy(q, j):
        return pltpu.make_async_remote_copy(
            src_ref=gst.at[q, lax.rem(j, SPAN)],
            dst_ref=out.at[j, me_slab],
            send_sem=grad_send.at[q, j],
            recv_sem=grad_recv.at[j, me_slab],
            device_id=holder(q, j),
            device_id_type=MESH,
        )

    own_copy = pltpu.make_async_copy(
        gst.at[me_slab, CENTER], out.at[CENTER, me_slab], own_sem
    )

    def send_grads(q):
        def one(j, carry):
            @pl.when(remote(q, j))
            def _():
                grad_copy(q, j).start()

            return carry

        lax.fori_loop(0, REACH, one, 0)

        @pl.when(q == me_slab)
        def _():
            own_copy.start()

    def backward(i, carry):
        s = slices - 1 - i
        leave(s)

        @pl.when(lax.rem(s, 2) == 0)
        def _():
            send_grads(s // 2)

        real, imag = waves[0], waves[1]
        layer_real, layer_imag = layer(s)
        real, imag = both_sides(
            tab, 1, 0,
            layer_real * real + layer_imag * imag,
            layer_real * imag - layer_imag * real,
        )
        waves[0] = real
        waves[1] = imag
        return carry

    lax.fori_loop(0, slices - 1, backward, 0, unroll=True)
    leave(0)
    send_grads(0)

    def finish_patch(i, carry):
        j, peer = patch_order(i)

        @pl.when(remote(peer, j))
        def _():
            patch_copy(j, peer).wait_send()

        return carry

    lax.fori_loop(0, count, finish_patch, 0)
    far_meas.wait_send()

    def finish_grad(i, carry):
        j, q = i // slabs, lax.rem(i, slabs)

        @pl.when(remote(q, j))
        def _():
            grad_copy(q, j).wait_send()
            pltpu.make_async_remote_copy(
                src_ref=gst.at[q, 0],
                dst_ref=out.at[j, q],
                send_sem=grad_send.at[q, j],
                recv_sem=grad_recv.at[j, q],
                device_id=worker(q, j),
                device_id_type=MESH,
            ).wait_recv()

        return carry

    lax.fori_loop(0, count, finish_grad, 0)
    own_copy.wait()


def update_kernel(slabs, strips, pos, pieces, obj, first, second, obj_out, first_out, second_out, grad):
    me_strip = lax.axis_index("strip")
    grad[...] = jnp.zeros_like(grad)
    shape = (2, 2, ROWS, PATCH)
    lane = lax.broadcasted_iota(jnp.int32, shape, 3)
    row = lax.broadcasted_iota(jnp.int32, shape, 2)

    def place(i, carry):
        j, k = i // slabs, lax.rem(i, slabs)
        owner = lax.rem(me_strip + strips - j, strips)
        item = owner * slabs + k
        column = pos[1, item]
        local_row = pos[0, item] - owner * ROWS
        low = jnp.where(j == 0, local_row, 0)
        high = jnp.where(j == SPAN, local_row, ROWS)
        tile = lax.shift_right_logical(column, 7)
        after = (tile + 1) & 15
        shift = column & 127
        piece = jnp.where((row >= low) & (row < high), pieces[j, k], 0.0)
        here = pl.ds(pl.multiple_of(tile * PATCH, PATCH), PATCH)
        there = pl.ds(pl.multiple_of(after * PATCH, PATCH), PATCH)
        grad[:, :, :, here] += jnp.where(lane >= shift, piece, 0.0)
        grad[:, :, :, there] += jnp.where(lane >= shift, 0.0, piece)
        return carry

    lax.fori_loop(0, REACH * slabs, place, 0)
    gradient = grad[...]
    first_new = beta_one * first[...] + (1.0 - beta_one) * gradient
    second_new = beta_two * second[...] + (1.0 - beta_two) * gradient * gradient
    first_hat = first_new / (1.0 - beta_one**adam_step)
    second_hat = second_new / (1.0 - beta_two**adam_step)
    obj_out[...] = obj[...] - learn_rate * first_hat / (jnp.sqrt(second_hat) + adam_eps)
    first_out[...] = first_new
    second_out[...] = second_new


def shards(slabs, strips, object_field, first_moment, second_moment, probe_wave, measured, positions, fresnel):
    vmem = pl.BlockSpec(memory_space=pltpu.VMEM)
    smem = pl.BlockSpec(memory_space=pltpu.SMEM)
    anywhere = pl.BlockSpec(memory_space=pl.ANY)
    f32 = jnp.float32
    count = REACH * slabs
    tiles = object_field.shape[3] // PATCH
    piece = (2, 2, ROWS, PATCH)
    pair = (2, PATCH, PATCH)
    turned = positions.T
    pieces = pl.pallas_call(
        functools.partial(wave_kernel, slabs, strips),
        out_shape=pltpu.VMEM((REACH, slabs) + piece, f32),
        in_specs=[pl.BlockSpec(memory_space=pltpu.HBM)] * 6,
        out_specs=pl.BlockSpec(memory_space=pltpu.VMEM),
        scratch_shapes=[
            pltpu.SMEM((2, positions.shape[0]), jnp.int32),
            pltpu.SMEM((1,), f32),
            pltpu.VMEM((tiles,) + piece, f32),
            pltpu.VMEM(pair, f32),
            pltpu.VMEM((PATCH, PATCH), f32),
            pltpu.VMEM(pair, f32),
            pltpu.VMEM((count,) + piece, f32),
            pltpu.VMEM((slabs, REACH) + piece, f32),
            pltpu.VMEM((4, 2, 2 * PATCH, 2 * PATCH), jnp.bfloat16),
            pltpu.VMEM((2 * slabs,) + pair, f32),
            pltpu.VMEM(pair, f32),
            pltpu.VMEM((slabs, SPAN) + piece, f32),
            pltpu.SemaphoreType.DMA((tiles,)),
            pltpu.SemaphoreType.DMA((4,)),
            pltpu.SemaphoreType.DMA((2,)),
            pltpu.SemaphoreType.DMA((count,)),
            pltpu.SemaphoreType.DMA((slabs, REACH)),
            pltpu.SemaphoreType.DMA((slabs, REACH)),
            pltpu.SemaphoreType.DMA((REACH, slabs)),
            pltpu.SemaphoreType.DMA(()),
        ],
        compiler_params=pltpu.CompilerParams(
            collective_id=0, has_side_effects=True, vmem_limit_bytes=61000000
        ),
    )(turned, fresnel, object_field, probe_wave, measured, fourier_table())
    like = jax.ShapeDtypeStruct(object_field.shape, f32)
    return pl.pallas_call(
        functools.partial(update_kernel, slabs, strips),
        out_shape=(like, like, like),
        in_specs=[smem, vmem, vmem, vmem, vmem],
        out_specs=(vmem, vmem, vmem),
        scratch_shapes=[pltpu.VMEM(object_field.shape, f32)],
        compiler_params=pltpu.CompilerParams(vmem_limit_bytes=12 << 20),
    )(turned, pieces, object_field, first_moment, second_moment)


def solution(mesh):
    spec = P(None, "slab", "strip", None)
    return jax.shard_map(
        functools.partial(shards, mesh.shape["slab"], mesh.shape["strip"]),
        mesh=mesh,
        in_specs=(spec, spec, spec, P(), P("strip", None, None), P(), P()),
        out_specs=(spec, spec, spec),
        check_vma=False,
    )
```

```python
import functools

import jax
import jax.numpy as jnp
import numpy as np
from jax import lax
from jax.experimental import pallas as pl
from jax.experimental.pallas import tpu as pltpu
from jax.sharding import PartitionSpec as P

beta_one = 0.9
beta_two = 0.999
learn_rate = 0.05
adam_eps = 1e-08
adam_step = 10.0

PATCH = 128
ROWS = 16
SPAN = PATCH // ROWS
REACH = SPAN + 1
CENTER = SPAN // 2
AHEAD = 6
MESH = pl.DeviceIdType.MESH


def fourier_table():
    index = np.arange(PATCH)
    angle = 2.0 * np.pi / PATCH * ((index[:, None] * index[None, :]) % PATCH)
    table = np.stack([np.cos(angle), -np.sin(angle)]) / np.sqrt(PATCH)
    return jnp.asarray(table.astype(np.float32))


def split(value):
    high = value.astype(jnp.bfloat16)
    low = (value - high.astype(jnp.float32)).astype(jnp.bfloat16)
    return high, low


def rolled(value, amount, axis, bits):
    for bit in range(bits):
        taken = jnp.broadcast_to((amount >> bit) & 1, value.shape) == 1
        value = jnp.where(taken, pltpu.roll(value, 1 << bit, axis), value)
    return value


def dot(left, right):
    return jnp.dot(left, right, preferred_element_type=jnp.float32)


def both_sides(tab, left, right, real, imag):
    high, low = split(jnp.concatenate([real, imag], axis=1))
    wide = dot(jnp.concatenate([high, low], axis=0), tab[right, 0])
    fine = dot(high, tab[right, 1])
    turned = wide[:PATCH] + wide[PATCH:] + fine
    high, low = split(jnp.concatenate([turned[:, :PATCH], turned[:, PATCH:]], axis=0))
    wide = dot(tab[left, 0], jnp.concatenate([high, low], axis=1))
    fine = dot(tab[left, 1], high)
    done = wide[:, :PATCH] + wide[:, PATCH:] + fine
    return done[:PATCH], done[PATCH:]


def fill_tables(tab, four, fresnel):
    four_real, four_imag = four[0], four[1]

    def phase(axis):
        index = lax.broadcasted_iota(jnp.int32, (PATCH, PATCH), axis)
        signed = jnp.where(index < PATCH // 2, index, index - PATCH).astype(jnp.float32)
        angle = fresnel * signed * signed
        return jnp.cos(angle), -jnp.sin(angle)

    def scaled(axis):
        real, imag = phase(axis)
        return four_real * real - four_imag * imag, four_real * imag + four_imag * real

    def put(slot, real, imag, sign):
        top = jnp.concatenate([real, -imag if sign > 0 else imag], axis=1)
        bottom = jnp.concatenate([imag if sign > 0 else -imag, real], axis=1)
        high, low = split(jnp.concatenate([top, bottom], axis=0))
        tab[slot, 0] = high
        tab[slot, 1] = low

    def full(left, right):
        return jnp.dot(
            left, right, precision=lax.Precision.HIGHEST, preferred_element_type=jnp.float32
        )

    far_real, far_imag = scaled(0)
    put(2, far_real, far_imag, 1)
    prop_real = full(four_real, far_real) + full(four_imag, far_imag)
    prop_imag = full(four_real, far_imag) - full(four_imag, far_real)
    put(0, prop_real, prop_imag, 1)
    put(1, prop_real, prop_imag, -1)
    put(3, *scaled(1), -1)


def wave_kernel(
    slabs, strips, pos_in, fresnel_in, obj_in, probe_in, meas_in, four_in, out,
    pos, fresnel, obj, probe, meas, four, stage, recv, tab, saved, waves, gst,
    tile_sem, load_sem, meas_sem, patch_send, patch_recv, grad_send, grad_recv, own_sem,
):
    me_slab = lax.axis_index("slab")
    me_strip = lax.axis_index("strip")
    count = REACH * slabs

    def moved(by):
        return lax.rem(me_strip + strips + by, strips)

    def worker(peer, j):
        return {"slab": peer, "strip": moved(CENTER - j)}

    def holder(peer, j):
        return {"slab": peer, "strip": moved(j - CENTER)}

    def remote(peer, j):
        return (peer != me_slab) | (j != CENTER)

    tiles = obj.shape[0]

    def tile_load(t):
        return pltpu.make_async_copy(
            obj_in.at[:, :, :, pl.ds(pl.multiple_of(t * PATCH, PATCH), PATCH)], obj.at[t], tile_sem.at[t]
        )

    def start_tile(t, carry):
        tile_load(t).start()
        return carry

    def wait_tile(t, carry):
        tile_load(t).wait()
        return carry

    pos_load = pltpu.make_async_copy(pos_in, pos, load_sem.at[2])
    pos_load.start()
    lax.fori_loop(0, tiles, start_tile, 0)
    loads = [
        pltpu.make_async_copy(probe_in, probe, load_sem.at[0]),
        pltpu.make_async_copy(four_in, four, load_sem.at[1]),
        pltpu.make_async_copy(fresnel_in, fresnel, load_sem.at[3]),
    ]
    for load in loads:
        load.start()

    barrier = pltpu.get_barrier_semaphore()

    def greet(i, carry):
        j, peer = i // slabs, lax.rem(i, slabs)

        @pl.when(remote(peer, j))
        def _():
            pl.semaphore_signal(
                barrier, inc=1, device_id=worker(peer, j), device_id_type=MESH
            )

        return carry

    lax.fori_loop(0, count, greet, 0)
    pos_load.wait()
    lax.fori_loop(0, tiles, wait_tile, 0)
    lane = lax.broadcasted_iota(jnp.int32, (2, 2, ROWS, PATCH), 3)

    def patch_order(i):
        return lax.rem(i, REACH), lax.rem(me_slab + i // REACH, slabs)

    def cut(i):
        j, peer = patch_order(i)
        item = moved(-j) * slabs + peer
        column = pos[1, item]
        tile = lax.shift_right_logical(column, 7)
        after = (tile + 1) & 15
        stage[j * slabs + peer] = jnp.where(lane >= (column & 127), obj[tile], obj[after])

    def cut_more(i, carry):
        cut(i)
        return carry

    def patch_copy(j, peer):
        return pltpu.make_async_remote_copy(
            src_ref=stage.at[j * slabs + peer],
            dst_ref=recv.at[me_slab, j],
            send_sem=patch_send.at[j * slabs + peer],
            recv_sem=patch_recv.at[me_slab, j],
            device_id=worker(peer, j),
            device_id_type=MESH,
        )

    def send_patch(i, carry):
        j, peer = patch_order(i)

        @pl.when(remote(peer, j))
        def _():
            patch_copy(j, peer).start()

        return carry

    lax.fori_loop(0, AHEAD, cut_more, 0)
    pl.semaphore_wait(barrier, count - 1)

    def cut_and_send(i, carry):
        send_patch(i, carry)
        cut(i + AHEAD)
        return carry

    lax.fori_loop(0, count - AHEAD, cut_and_send, 0)
    lax.fori_loop(count - AHEAD, count, send_patch, 0)
    far_meas = pltpu.make_async_remote_copy(
        src_ref=meas_in.at[me_slab],
        dst_ref=meas,
        send_sem=meas_sem.at[0],
        recv_sem=meas_sem.at[1],
        device_id={"slab": me_slab, "strip": moved(CENTER)},
        device_id_type=MESH,
    )
    far_meas.start()
    recv[me_slab, CENTER] = stage[CENTER * slabs + me_slab]

    for load in loads:
        load.wait()
    fill_tables(tab, four, fresnel[0])
    owner = moved(-CENTER)
    own = owner * slabs + me_slab
    own_row = pos[0, own] - owner * ROWS
    own_shift = pos[1, own] & 127
    for part in range(2):
        waves[part] = rolled(rolled(probe[part], own_row, 0, 4), own_shift, 1, 7)
    row = lax.broadcasted_iota(jnp.int32, (ROWS, PATCH), 0)

    def arrived(q):
        def one(j, carry):
            @pl.when(remote(q, j))
            def _():
                pltpu.make_async_remote_copy(
                    src_ref=stage.at[0],
                    dst_ref=recv.at[q, j],
                    send_sem=patch_send.at[0],
                    recv_sem=patch_recv.at[q, j],
                    device_id=holder(q, j),
                    device_id_type=MESH,
                ).wait_recv()

            return carry

        lax.fori_loop(0, REACH, one, 0)

    def layer(s):
        q, n = s // 2, lax.rem(s, 2)
        parts = []
        for part in range(2):
            first = jnp.where(row >= own_row, recv[q, 0, part, n], recv[q, SPAN, part, n])
            rest = [recv[q, j, part, n] for j in range(1, SPAN)]
            parts.append(jnp.concatenate([first] + rest, axis=0))
        return parts

    def enter(s):
        real, imag = waves[0], waves[1]
        saved[s, 0] = real
        saved[s, 1] = imag
        layer_real, layer_imag = layer(s)
        return (
            real * layer_real - imag * layer_imag,
            real * layer_imag + imag * layer_real,
        )

    def forward(s, carry):
        @pl.when(lax.rem(s, 2) == 0)
        def _():
            arrived(s // 2)

        real, imag = both_sides(tab, 0, 1, *enter(s))
        waves[0] = real
        waves[1] = imag
        return carry

    slices = 2 * slabs
    lax.fori_loop(0, slices - 1, forward, 0, unroll=True)
    real, imag = both_sides(tab, 2, 3, *enter(slices - 1))

    far_meas.wait_recv()
    factor = 2.0 * (real * real + imag * imag - meas[...])
    real, imag = both_sides(tab, 3, 2, real * factor, imag * factor)
    waves[0] = real
    waves[1] = imag

    def leave(s):
        q, n = s // 2, lax.rem(s, 2)
        real, imag = waves[0], waves[1]
        old_real, old_imag = saved[s, 0], saved[s, 1]
        grad_real = old_real * real + old_imag * imag
        grad_imag = old_real * imag - old_imag * real
        for j in range(SPAN):
            gst[q, j, 0, n] = grad_real[j * ROWS : (j + 1) * ROWS]
            gst[q, j, 1, n] = grad_imag[j * ROWS : (j + 1) * ROWS]

    def grad_copy(q, j):
        return pltpu.make_async_remote_copy(
            src_ref=gst.at[q, lax.rem(j, SPAN)],
            dst_ref=out.at[j, me_slab],
            send_sem=grad_send.at[q, j],
            recv_sem=grad_recv.at[j, me_slab],
            device_id=holder(q, j),
            device_id_type=MESH,
        )

    own_copy = pltpu.make_async_copy(
        gst.at[me_slab, CENTER], out.at[CENTER, me_slab], own_sem
    )

    def send_grads(q):
        def one(j, carry):
            @pl.when(remote(q, j))
            def _():
                grad_copy(q, j).start()

            return carry

        lax.fori_loop(0, REACH, one, 0)

        @pl.when(q == me_slab)
        def _():
            own_copy.start()

    def backward(i, carry):
        s = slices - 1 - i
        leave(s)

        @pl.when(lax.rem(s, 2) == 0)
        def _():
            send_grads(s // 2)

        real, imag = waves[0], waves[1]
        layer_real, layer_imag = layer(s)
        real, imag = both_sides(
            tab, 1, 0,
            layer_real * real + layer_imag * imag,
            layer_real * imag - layer_imag * real,
        )
        waves[0] = real
        waves[1] = imag
        return carry

    lax.fori_loop(0, slices - 1, backward, 0, unroll=True)
    leave(0)
    send_grads(0)

    def finish_patch(i, carry):
        j, peer = patch_order(i)

        @pl.when(remote(peer, j))
        def _():
            patch_copy(j, peer).wait_send()

        return carry

    lax.fori_loop(0, count, finish_patch, 0)
    far_meas.wait_send()

    def finish_grad(i, carry):
        j, q = i // slabs, lax.rem(i, slabs)

        @pl.when(remote(q, j))
        def _():
            grad_copy(q, j).wait_send()
            pltpu.make_async_remote_copy(
                src_ref=gst.at[q, 0],
                dst_ref=out.at[j, q],
                send_sem=grad_send.at[q, j],
                recv_sem=grad_recv.at[j, q],
                device_id=worker(q, j),
                device_id_type=MESH,
            ).wait_recv()

        return carry

    lax.fori_loop(0, count, finish_grad, 0)
    own_copy.wait()


def update_kernel(slabs, strips, pos, pieces, obj, first, second, obj_out, first_out, second_out, grad, done, out_sem):
    me_strip = lax.axis_index("strip")
    grad[...] = jnp.zeros_like(grad)
    shape = (2, 2, ROWS, PATCH)
    lane = lax.broadcasted_iota(jnp.int32, shape, 3)
    row = lax.broadcasted_iota(jnp.int32, shape, 2)

    def place(i, carry):
        j, k = i // slabs, lax.rem(i, slabs)
        owner = lax.rem(me_strip + strips - j, strips)
        item = owner * slabs + k
        column = pos[1, item]
        local_row = pos[0, item] - owner * ROWS
        low = jnp.where(j == 0, local_row, 0)
        high = jnp.where(j == SPAN, local_row, ROWS)
        tile = lax.shift_right_logical(column, 7)
        after = (tile + 1) & 15
        shift = column & 127
        piece = jnp.where((row >= low) & (row < high), pieces[j, k], 0.0)
        here = pl.ds(pl.multiple_of(tile * PATCH, PATCH), PATCH)
        there = pl.ds(pl.multiple_of(after * PATCH, PATCH), PATCH)
        grad[:, :, :, here] += jnp.where(lane >= shift, piece, 0.0)
        grad[:, :, :, there] += jnp.where(lane >= shift, 0.0, piece)
        return carry

    lax.fori_loop(0, REACH * slabs, place, 0, unroll=4)
    copies = []
    for part in range(2):
        for n in range(2):
            gradient = grad[part, n]
            first_new = beta_one * first[part, n] + (1.0 - beta_one) * gradient
            second_new = beta_two * second[part, n] + (1.0 - beta_two) * gradient * gradient
            first_hat = first_new / (1.0 - beta_one**adam_step)
            second_hat = second_new / (1.0 - beta_two**adam_step)
            done[0, part, n] = obj[part, n] - learn_rate * first_hat / (
                jnp.sqrt(second_hat) + adam_eps
            )
            done[1, part, n] = first_new
            done[2, part, n] = second_new
            for slot, target in enumerate((obj_out, first_out, second_out)):
                copies.append(
                    pltpu.make_async_copy(
                        done.at[slot, part, n], target.at[part, n], out_sem.at[slot, part, n]
                    )
                )
                copies[-1].start()
    for copy in copies:
        copy.wait()


def shards(slabs, strips, object_field, first_moment, second_moment, probe_wave, measured, positions, fresnel):
    vmem = pl.BlockSpec(memory_space=pltpu.VMEM)
    smem = pl.BlockSpec(memory_space=pltpu.SMEM)
    anywhere = pl.BlockSpec(memory_space=pl.ANY)
    f32 = jnp.float32
    count = REACH * slabs
    tiles = object_field.shape[3] // PATCH
    piece = (2, 2, ROWS, PATCH)
    pair = (2, PATCH, PATCH)
    turned = positions.T
    pieces = pl.pallas_call(
        functools.partial(wave_kernel, slabs, strips),
        out_shape=pltpu.VMEM((REACH, slabs) + piece, f32),
        in_specs=[pl.BlockSpec(memory_space=pltpu.HBM)] * 6,
        out_specs=pl.BlockSpec(memory_space=pltpu.VMEM),
        scratch_shapes=[
            pltpu.SMEM((2, positions.shape[0]), jnp.int32),
            pltpu.SMEM((1,), f32),
            pltpu.VMEM((tiles,) + piece, f32),
            pltpu.VMEM(pair, f32),
            pltpu.VMEM((PATCH, PATCH), f32),
            pltpu.VMEM(pair, f32),
            pltpu.VMEM((count,) + piece, f32),
            pltpu.VMEM((slabs, REACH) + piece, f32),
            pltpu.VMEM((4, 2, 2 * PATCH, 2 * PATCH), jnp.bfloat16),
            pltpu.VMEM((2 * slabs,) + pair, f32),
            pltpu.VMEM(pair, f32),
            pltpu.VMEM((slabs, SPAN) + piece, f32),
            pltpu.SemaphoreType.DMA((tiles,)),
            pltpu.SemaphoreType.DMA((4,)),
            pltpu.SemaphoreType.DMA((2,)),
            pltpu.SemaphoreType.DMA((count,)),
            pltpu.SemaphoreType.DMA((slabs, REACH)),
            pltpu.SemaphoreType.DMA((slabs, REACH)),
            pltpu.SemaphoreType.DMA((REACH, slabs)),
            pltpu.SemaphoreType.DMA(()),
        ],
        compiler_params=pltpu.CompilerParams(
            collective_id=0, has_side_effects=True, vmem_limit_bytes=61000000
        ),
    )(turned, fresnel, object_field, probe_wave, measured, fourier_table())
    like = jax.ShapeDtypeStruct(object_field.shape, f32)
    return pl.pallas_call(
        functools.partial(update_kernel, slabs, strips),
        out_shape=(like, like, like),
        in_specs=[smem, vmem, vmem, vmem, vmem],
        out_specs=(anywhere, anywhere, anywhere),
        scratch_shapes=[
            pltpu.VMEM(object_field.shape, f32),
            pltpu.VMEM((3,) + object_field.shape, f32),
            pltpu.SemaphoreType.DMA((3, 2, 2)),
        ],
        compiler_params=pltpu.CompilerParams(vmem_limit_bytes=12 << 20),
    )(turned, pieces, object_field, first_moment, second_moment)


def solution(mesh):
    spec = P(None, "slab", "strip", None)
    return jax.shard_map(
        functools.partial(shards, mesh.shape["slab"], mesh.shape["strip"]),
        mesh=mesh,
        in_specs=(spec, spec, spec, P(), P("strip", None, None), P(), P()),
        out_specs=(spec, spec, spec),
        check_vma=False,
    )
```

```python
import functools

import jax
import jax.numpy as jnp
import numpy as np
from jax import lax
from jax.experimental import pallas as pl
from jax.experimental.pallas import tpu as pltpu
from jax.sharding import PartitionSpec as P

beta_one = 0.9
beta_two = 0.999
learn_rate = 0.05
adam_eps = 1e-08
adam_step = 10.0

PATCH = 128
ROWS = 16
SPAN = PATCH // ROWS
REACH = SPAN + 1
CENTER = SPAN // 2
AHEAD = 6
MESH = pl.DeviceIdType.MESH


def fourier_table():
    index = np.arange(PATCH)
    angle = 2.0 * np.pi / PATCH * ((index[:, None] * index[None, :]) % PATCH)
    table = np.stack([np.cos(angle), -np.sin(angle)]) / np.sqrt(PATCH)
    return jnp.asarray(table.astype(np.float32))


def split(value):
    high = value.astype(jnp.bfloat16)
    low = (value - high.astype(jnp.float32)).astype(jnp.bfloat16)
    return high, low


def rolled(value, amount, axis, bits):
    for bit in range(bits):
        taken = jnp.broadcast_to((amount >> bit) & 1, value.shape) == 1
        value = jnp.where(taken, pltpu.roll(value, 1 << bit, axis), value)
    return value


def dot(left, right):
    return jnp.dot(left, right, preferred_element_type=jnp.float32)


def both_sides(tab, left, right, real, imag):
    high, low = split(jnp.concatenate([real, imag], axis=1))
    wide = dot(jnp.concatenate([high, low], axis=0), tab[right, 0])
    fine = dot(high, tab[right, 1])
    turned = wide[:PATCH] + wide[PATCH:] + fine
    high, low = split(jnp.concatenate([turned[:, :PATCH], turned[:, PATCH:]], axis=0))
    wide = dot(tab[left, 0], jnp.concatenate([high, low], axis=1))
    fine = dot(tab[left, 1], high)
    done = wide[:, :PATCH] + wide[:, PATCH:] + fine
    return done[:PATCH], done[PATCH:]


def fill_tables(tab, four, fresnel):
    four_real, four_imag = four[0], four[1]

    def phase(axis):
        index = lax.broadcasted_iota(jnp.int32, (PATCH, PATCH), axis)
        signed = jnp.where(index < PATCH // 2, index, index - PATCH).astype(jnp.float32)
        angle = fresnel * signed * signed
        return jnp.cos(angle), -jnp.sin(angle)

    def scaled(axis):
        real, imag = phase(axis)
        return four_real * real - four_imag * imag, four_real * imag + four_imag * real

    def put(slot, real, imag, sign):
        top = jnp.concatenate([real, -imag if sign > 0 else imag], axis=1)
        bottom = jnp.concatenate([imag if sign > 0 else -imag, real], axis=1)
        high, low = split(jnp.concatenate([top, bottom], axis=0))
        tab[slot, 0] = high
        tab[slot, 1] = low

    def full(left, right):
        return jnp.dot(
            left, right, precision=lax.Precision.HIGHEST, preferred_element_type=jnp.float32
        )

    far_real, far_imag = scaled(0)
    put(2, far_real, far_imag, 1)
    prop_real = full(four_real, far_real) + full(four_imag, far_imag)
    prop_imag = full(four_real, far_imag) - full(four_imag, far_real)
    put(0, prop_real, prop_imag, 1)
    put(1, prop_real, prop_imag, -1)
    put(3, *scaled(1), -1)


def wave_kernel(
    slabs, strips, pos_in, fresnel_in, obj_in, probe_in, meas_in, four_in, out,
    pos, fresnel, obj, probe, meas, four, stage, recv, tab, saved, waves, gst,
    tile_sem, load_sem, meas_sem, patch_send, patch_recv, grad_send, grad_recv, own_sem,
):
    me_slab = lax.axis_index("slab")
    me_strip = lax.axis_index("strip")
    count = REACH * slabs

    def moved(by):
        return lax.rem(me_strip + strips + by, strips)

    def worker(peer, j):
        return {"slab": peer, "strip": moved(CENTER - j)}

    def holder(peer, j):
        return {"slab": peer, "strip": moved(j - CENTER)}

    def remote(peer, j):
        return (peer != me_slab) | (j != CENTER)

    tiles = obj.shape[0]

    def tile_load(t):
        return pltpu.make_async_copy(
            obj_in.at[:, :, :, pl.ds(pl.multiple_of(t * PATCH, PATCH), PATCH)], obj.at[t], tile_sem.at[t]
        )

    def start_tile(t, carry):
        tile_load(t).start()
        return carry

    def wait_tile(t, carry):
        tile_load(t).wait()
        return carry

    pos_load = pltpu.make_async_copy(pos_in, pos, load_sem.at[2])
    pos_load.start()
    lax.fori_loop(0, tiles, start_tile, 0)
    loads = [
        pltpu.make_async_copy(probe_in, probe, load_sem.at[0]),
        pltpu.make_async_copy(four_in, four, load_sem.at[1]),
        pltpu.make_async_copy(fresnel_in, fresnel, load_sem.at[3]),
    ]
    for load in loads:
        load.start()

    barrier = pltpu.get_barrier_semaphore()

    def greet(i, carry):
        j, peer = i // slabs, lax.rem(i, slabs)

        @pl.when(remote(peer, j))
        def _():
            pl.semaphore_signal(
                barrier, inc=1, device_id=worker(peer, j), device_id_type=MESH
            )

        return carry

    lax.fori_loop(0, count, greet, 0)
    pos_load.wait()
    lax.fori_loop(0, tiles, wait_tile, 0)
    lane = lax.broadcasted_iota(jnp.int32, (2, 2, ROWS, PATCH), 3)

    def patch_order(i):
        return lax.rem(i, REACH), lax.rem(me_slab + i // REACH, slabs)

    def cut(i):
        j, peer = patch_order(i)
        item = moved(-j) * slabs + peer
        column = pos[1, item]
        tile = lax.shift_right_logical(column, 7)
        after = (tile + 1) & 15
        stage[j * slabs + peer] = jnp.where(lane >= (column & 127), obj[tile], obj[after])

    def cut_more(i, carry):
        cut(i)
        return carry

    def patch_copy(j, peer):
        return pltpu.make_async_remote_copy(
            src_ref=stage.at[j * slabs + peer],
            dst_ref=recv.at[me_slab, j],
            send_sem=patch_send.at[j * slabs + peer],
            recv_sem=patch_recv.at[me_slab, j],
            device_id=worker(peer, j),
            device_id_type=MESH,
        )

    def send_patch(i, carry):
        j, peer = patch_order(i)

        @pl.when(remote(peer, j))
        def _():
            patch_copy(j, peer).start()

        return carry

    lax.fori_loop(0, AHEAD, cut_more, 0)
    pl.semaphore_wait(barrier, count - 1)

    def cut_and_send(i, carry):
        send_patch(i, carry)
        cut(i + AHEAD)
        return carry

    lax.fori_loop(0, count - AHEAD, cut_and_send, 0)
    lax.fori_loop(count - AHEAD, count, send_patch, 0)
    far_meas = pltpu.make_async_remote_copy(
        src_ref=meas_in.at[me_slab],
        dst_ref=meas,
        send_sem=meas_sem.at[0],
        recv_sem=meas_sem.at[1],
        device_id={"slab": me_slab, "strip": moved(CENTER)},
        device_id_type=MESH,
    )
    far_meas.start()
    recv[me_slab, CENTER] = stage[CENTER * slabs + me_slab]

    for load in loads:
        load.wait()
    fill_tables(tab, four, fresnel[0])
    owner = moved(-CENTER)
    own = owner * slabs + me_slab
    own_row = pos[0, own] - owner * ROWS
    own_shift = pos[1, own] & 127
    for part in range(2):
        waves[part] = rolled(rolled(probe[part], own_row, 0, 4), own_shift, 1, 7)
    row = lax.broadcasted_iota(jnp.int32, (ROWS, PATCH), 0)

    def arrived(q):
        def one(j, carry):
            @pl.when(remote(q, j))
            def _():
                pltpu.make_async_remote_copy(
                    src_ref=stage.at[0],
                    dst_ref=recv.at[q, j],
                    send_sem=patch_send.at[0],
                    recv_sem=patch_recv.at[q, j],
                    device_id=holder(q, j),
                    device_id_type=MESH,
                ).wait_recv()

            return carry

        lax.fori_loop(0, REACH, one, 0)

    def layer(s):
        q, n = s // 2, lax.rem(s, 2)
        parts = []
        for part in range(2):
            first = jnp.where(row >= own_row, recv[q, 0, part, n], recv[q, SPAN, part, n])
            rest = [recv[q, j, part, n] for j in range(1, SPAN)]
            parts.append(jnp.concatenate([first] + rest, axis=0))
        return parts

    def enter(s):
        real, imag = waves[0], waves[1]
        saved[s, 0] = real
        saved[s, 1] = imag
        layer_real, layer_imag = layer(s)
        return (
            real * layer_real - imag * layer_imag,
            real * layer_imag + imag * layer_real,
        )

    def forward(s, carry):
        @pl.when(lax.rem(s, 2) == 0)
        def _():
            arrived(s // 2)

        real, imag = both_sides(tab, 0, 1, *enter(s))
        waves[0] = real
        waves[1] = imag
        return carry

    slices = 2 * slabs
    lax.fori_loop(0, slices - 1, forward, 0, unroll=True)
    real, imag = both_sides(tab, 2, 3, *enter(slices - 1))

    far_meas.wait_recv()
    factor = 2.0 * (real * real + imag * imag - meas[...])
    real, imag = both_sides(tab, 3, 2, real * factor, imag * factor)
    waves[0] = real
    waves[1] = imag

    def leave(s):
        q, n = s // 2, lax.rem(s, 2)
        real, imag = waves[0], waves[1]
        old_real, old_imag = saved[s, 0], saved[s, 1]
        grad_real = old_real * real + old_imag * imag
        grad_imag = old_real * imag - old_imag * real
        for j in range(SPAN):
            gst[q, j, 0, n] = grad_real[j * ROWS : (j + 1) * ROWS]
            gst[q, j, 1, n] = grad_imag[j * ROWS : (j + 1) * ROWS]

    def grad_copy(q, j, n):
        return pltpu.make_async_remote_copy(
            src_ref=gst.at[q, lax.rem(j, SPAN), :, n],
            dst_ref=out.at[j, me_slab, :, n],
            send_sem=grad_send.at[q, j, n],
            recv_sem=grad_recv.at[j, me_slab, n],
            device_id=holder(q, j),
            device_id_type=MESH,
        )

    own_copy = pltpu.make_async_copy(
        gst.at[me_slab, CENTER], out.at[CENTER, me_slab], own_sem
    )

    def send_grads(q, n):
        def one(j, carry):
            @pl.when(remote(q, j))
            def _():
                grad_copy(q, j, n).start()

            return carry

        lax.fori_loop(0, REACH, one, 0)

        @pl.when((q == me_slab) & (n == 0))
        def _():
            own_copy.start()

    def backward(i, carry):
        s = slices - 1 - i
        leave(s)

        send_grads(s // 2, lax.rem(s, 2))

        real, imag = waves[0], waves[1]
        layer_real, layer_imag = layer(s)
        real, imag = both_sides(
            tab, 1, 0,
            layer_real * real + layer_imag * imag,
            layer_real * imag - layer_imag * real,
        )
        waves[0] = real
        waves[1] = imag
        return carry

    lax.fori_loop(0, slices - 1, backward, 0, unroll=True)
    leave(0)
    send_grads(0, 0)

    def finish_patch(i, carry):
        j, peer = patch_order(i)

        @pl.when(remote(peer, j))
        def _():
            patch_copy(j, peer).wait_send()

        return carry

    lax.fori_loop(0, count, finish_patch, 0)
    far_meas.wait_send()

    def finish_grad(i, carry):
        j, q = i // slabs, lax.rem(i, slabs)

        @pl.when(remote(q, j))
        def _():
            for n in range(2):
                grad_copy(q, j, n).wait_send()
                pltpu.make_async_remote_copy(
                    src_ref=gst.at[q, 0, :, n],
                    dst_ref=out.at[j, q, :, n],
                    send_sem=grad_send.at[q, j, n],
                    recv_sem=grad_recv.at[j, q, n],
                    device_id=worker(q, j),
                    device_id_type=MESH,
                ).wait_recv()

        return carry

    lax.fori_loop(0, count, finish_grad, 0)
    own_copy.wait()


def update_kernel(slabs, strips, pos, pieces, obj, first, second, obj_out, first_out, second_out, grad, done, out_sem):
    me_strip = lax.axis_index("strip")
    grad[...] = jnp.zeros_like(grad)
    shape = (2, 2, ROWS, PATCH)
    lane = lax.broadcasted_iota(jnp.int32, shape, 3)
    row = lax.broadcasted_iota(jnp.int32, shape, 2)

    def place(i, carry):
        j, k = i // slabs, lax.rem(i, slabs)
        owner = lax.rem(me_strip + strips - j, strips)
        item = owner * slabs + k
        column = pos[1, item]
        local_row = pos[0, item] - owner * ROWS
        low = jnp.where(j == 0, local_row, 0)
        high = jnp.where(j == SPAN, local_row, ROWS)
        tile = lax.shift_right_logical(column, 7)
        after = (tile + 1) & 15
        shift = column & 127
        piece = jnp.where((row >= low) & (row < high), pieces[j, k], 0.0)
        here = pl.ds(pl.multiple_of(tile * PATCH, PATCH), PATCH)
        there = pl.ds(pl.multiple_of(after * PATCH, PATCH), PATCH)
        grad[:, :, :, here] += jnp.where(lane >= shift, piece, 0.0)
        grad[:, :, :, there] += jnp.where(lane >= shift, 0.0, piece)
        return carry

    lax.fori_loop(0, REACH * slabs, place, 0, unroll=4)
    copies = []
    for part in range(2):
        for n in range(2):
            gradient = grad[part, n]
            first_new = beta_one * first[part, n] + (1.0 - beta_one) * gradient
            second_new = beta_two * second[part, n] + (1.0 - beta_two) * gradient * gradient
            first_hat = first_new / (1.0 - beta_one**adam_step)
            second_hat = second_new / (1.0 - beta_two**adam_step)
            done[0, part, n] = obj[part, n] - learn_rate * first_hat / (
                jnp.sqrt(second_hat) + adam_eps
            )
            done[1, part, n] = first_new
            done[2, part, n] = second_new
            for slot, target in enumerate((obj_out, first_out, second_out)):
                copies.append(
                    pltpu.make_async_copy(
                        done.at[slot, part, n], target.at[part, n], out_sem.at[slot, part, n]
                    )
                )
                copies[-1].start()
    for copy in copies:
        copy.wait()


def shards(slabs, strips, object_field, first_moment, second_moment, probe_wave, measured, positions, fresnel):
    vmem = pl.BlockSpec(memory_space=pltpu.VMEM)
    smem = pl.BlockSpec(memory_space=pltpu.SMEM)
    anywhere = pl.BlockSpec(memory_space=pl.ANY)
    f32 = jnp.float32
    count = REACH * slabs
    tiles = object_field.shape[3] // PATCH
    piece = (2, 2, ROWS, PATCH)
    pair = (2, PATCH, PATCH)
    turned = positions.T
    pieces = pl.pallas_call(
        functools.partial(wave_kernel, slabs, strips),
        out_shape=pltpu.VMEM((REACH, slabs) + piece, f32),
        in_specs=[pl.BlockSpec(memory_space=pltpu.HBM)] * 6,
        out_specs=pl.BlockSpec(memory_space=pltpu.VMEM),
        scratch_shapes=[
            pltpu.SMEM((2, positions.shape[0]), jnp.int32),
            pltpu.SMEM((1,), f32),
            pltpu.VMEM((tiles,) + piece, f32),
            pltpu.VMEM(pair, f32),
            pltpu.VMEM((PATCH, PATCH), f32),
            pltpu.VMEM(pair, f32),
            pltpu.VMEM((count,) + piece, f32),
            pltpu.VMEM((slabs, REACH) + piece, f32),
            pltpu.VMEM((4, 2, 2 * PATCH, 2 * PATCH), jnp.bfloat16),
            pltpu.VMEM((2 * slabs,) + pair, f32),
            pltpu.VMEM(pair, f32),
            pltpu.VMEM((slabs, SPAN) + piece, f32),
            pltpu.SemaphoreType.DMA((tiles,)),
            pltpu.SemaphoreType.DMA((4,)),
            pltpu.SemaphoreType.DMA((2,)),
            pltpu.SemaphoreType.DMA((count,)),
            pltpu.SemaphoreType.DMA((slabs, REACH)),
            pltpu.SemaphoreType.DMA((slabs, REACH, 2)),
            pltpu.SemaphoreType.DMA((REACH, slabs, 2)),
            pltpu.SemaphoreType.DMA(()),
        ],
        compiler_params=pltpu.CompilerParams(
            collective_id=0, has_side_effects=True, vmem_limit_bytes=61000000
        ),
    )(turned, fresnel, object_field, probe_wave, measured, fourier_table())
    like = jax.ShapeDtypeStruct(object_field.shape, f32)
    return pl.pallas_call(
        functools.partial(update_kernel, slabs, strips),
        out_shape=(like, like, like),
        in_specs=[smem, vmem, vmem, vmem, vmem],
        out_specs=(anywhere, anywhere, anywhere),
        scratch_shapes=[
            pltpu.VMEM(object_field.shape, f32),
            pltpu.VMEM((3,) + object_field.shape, f32),
            pltpu.SemaphoreType.DMA((3, 2, 2)),
        ],
        compiler_params=pltpu.CompilerParams(vmem_limit_bytes=12 << 20),
    )(turned, pieces, object_field, first_moment, second_moment)


def solution(mesh):
    spec = P(None, "slab", "strip", None)
    return jax.shard_map(
        functools.partial(shards, mesh.shape["slab"], mesh.shape["strip"]),
        mesh=mesh,
        in_specs=(spec, spec, spec, P(), P("strip", None, None), P(), P()),
        out_specs=(spec, spec, spec),
        check_vma=False,
    )
```
